32 devices in a mesh: orb: 8 (over z, y), clu: 4 (over x, core).
Axes of the slice: x: 2, y: 2, z: 4, core: 2. Of those that a mesh axis runs over, the one named last changes fastest.
Arguments:
- integrals: bfloat16 [1024, 1024, 512], P('orb', 'clu'), may hold values from -1.1953125 to 1.1953125
- metric: bfloat16 [1024, 1024], P(None, 'orb'), may hold values from -0.1875 to 0.1875
- occ_energy: float32 [1024], replicated, may hold values from -2 to -0.5
- virt_energy: float32 [512], replicated, may hold values from 0.5 to 4
- orbital_order: int32 [4, 256], replicated, may hold values from 0 to 255, each once within a row
- pair_first: int32 [4, 8, 4], P('clu', 'orb'), may hold values from 0 to 31
- pair_second: int32 [4, 8, 4], replicated, may hold values from 0 to 255
- pair_live: int32 [4, 8, 4], P('clu', 'orb'), may hold values 0 or 1
Outputs:
- gamma: bfloat16 [1024, 1024, 512], P('orb', 'clu')
The draws below stay inside these ranges and needn't reach their ends.
Inputs may be any that keep to these rules, and one draw needn't show every extreme that they name: `orbital_order`: each row is a permutation of 0 to 255. `pair_second`: slot s names an orbital of cluster s.
All inputs are finite; a program needn't handle non-finite values. No bound on the sum of `pair_live` on one device may be relied on, other than what follows from the above.
Results may differ from the reference program's by a relative error of at most 0.0052.
Values may be sent and summed in bfloat16 or wider, within the bound.
A program may use at most 256 MiB of HBM per device.

```python
import math
import jax
import jax.numpy as jnp
import numpy as np
from jax import lax

X = 1024
OCC = 256
V = 512
PER_CLU = 1
ORBITALS = 1024
OD = 32
PAIRS = 4
N_ORB = 8
N_CLU = 4


def set_ends(result, key, smallest, top_value):
    spot = [jax.random.randint(jax.random.fold_in(key, axis), (), 0, length) for axis, length in enumerate(result.shape)]
    longest = result.shape.index(max(result.shape))
    next_to = spot[:longest] + [(spot[longest] + 1) % result.shape[longest]] + spot[longest + 1:]
    return result.at[tuple(spot)].set(smallest).at[tuple(next_to)].set(top_value)


def block_levels(own_key, extent, shards, least, high):
    factor_of = 1.0
    for position, parts in shards:
        steps = jax.random.uniform(jax.random.fold_in(jax.random.fold_in(own_key, 6), position), (parts,), jnp.float32, least / len(shards), high / len(shards))
        factor_of = factor_of * jnp.repeat(jnp.exp(steps), extent[position] // parts).reshape((-1,) + (1,) * (len(extent) - 1 - position))
    return factor_of


def rank_bounds(count, skew):
    portions = [(1 << 20) // math.isqrt(standing ** skew) + 1 for standing in range(1, count + 1)]
    scale = 1 + sum(portions) // (1 << 30)
    return np.cumsum(np.array([max(1, weight // scale) for weight in portions]))


def skewed_ids(stream_key, dims, amount, slope):
    listing = rank_bounds(amount, slope)
    ticket = jax.random.randint(jax.random.fold_in(stream_key, 1), dims, 0, int(listing[amount - 1]))
    grade = jnp.searchsorted(jnp.asarray(listing, jnp.int32), ticket, side="right")
    return jax.random.permutation(jax.random.fold_in(stream_key, 2), amount)[grade].astype(jnp.int32)


def scatter_about(rng, dims, deviation, limit, split=(), held_as=jnp.bfloat16):
    array = jax.random.normal(rng, dims, jnp.float32) * deviation
    if len(split) > 0:
        array = block_levels(rng, dims, split, -0.22, 0.18) * array
    return jnp.clip(array, min=-limit, max=limit).astype(held_as)


def setup_inputs(seed: int = 0) -> dict:
    keys = jax.random.split(jax.random.key(seed), 9)
    integrals = scatter_about(keys[0], (X, ORBITALS, V), 0.2, 1.1953125, ((0, 8), (1, 4)))
    metric = scatter_about(keys[1], (X, X), X ** -0.5, 0.1875, ((1, 8),))
    occ_energy = jnp.clip(jax.random.uniform(keys[2], (ORBITALS,), jnp.float32, -2.0, -0.5), -2.0, -0.5)
    virt_energy = jnp.clip(jax.random.uniform(keys[3], (V,), jnp.float32, 0.5, 4.0), 0.5, 4.0)
    orbital_order = jax.vmap(lambda own: jax.random.permutation(own, OCC))(jax.random.split(keys[4], N_CLU)).reshape((N_CLU, OCC)).astype(jnp.int32)
    pair_first = set_ends(jax.random.randint(keys[5], (N_CLU, N_ORB, PAIRS), 0, OD), jax.random.fold_in(keys[5], 1), 0, OD - 1).astype(jnp.int32)
    pair_second = set_ends(skewed_ids(keys[6], (N_CLU, N_ORB, PAIRS), OCC, 2), jax.random.fold_in(keys[6], 3), 0, OCC - 1).astype(jnp.int32)
    pair_live = set_ends((jax.random.randint(keys[7], (N_CLU, N_ORB, PAIRS), 0, 4) < 3).astype(jnp.int32), jax.random.fold_in(keys[7], 1), 0, 1)
    return dict(integrals=integrals, metric=metric, occ_energy=occ_energy, virt_energy=virt_energy, orbital_order=orbital_order, pair_first=pair_first, pair_second=pair_second, pair_live=pair_live)


def reference(integrals, metric, occ_energy, virt_energy, orbital_order, pair_first, pair_second, pair_live):
    owned_count = OCC // N_ORB
    fitted_blocks = []
    for cluster in range(N_CLU):
        cluster_rows = integrals[:, cluster * OCC:(cluster + 1) * OCC, :].reshape(X, OCC * V)
        product = jnp.dot(metric.T, cluster_rows, preferred_element_type=jnp.float32)
        fitted_blocks.append(product.astype(jnp.bfloat16).reshape(X, OCC, V))
    fitted = jnp.concatenate(fitted_blocks, axis=1)
    slot_cluster = (jnp.arange(PAIRS, dtype=jnp.int32) // PER_CLU).astype(jnp.int32)

    def device_gamma(device_index):
        cluster = device_index // N_ORB
        orb_column = device_index % N_ORB
        order_row = orbital_order[cluster]
        owned_orbs = lax.dynamic_slice_in_dim(order_row, orb_column * owned_count, owned_count) + cluster * OCC
        first_slot = pair_first[cluster, orb_column]
        second_orb = pair_second[cluster, orb_column] + slot_cluster * OCC
        live_mask = pair_live[cluster, orb_column].astype(jnp.float32)
        first_orb = jnp.take(owned_orbs, first_slot)
        first_fit = jnp.take(fitted, first_orb, axis=1).astype(jnp.float32)
        second_fit = jnp.take(fitted, second_orb, axis=1).astype(jnp.float32)
        intersection = jnp.einsum("xpa,xpb->pab", first_fit, second_fit)
        denominator = (virt_energy[None, :, None] + virt_energy[None, None, :]
                       - occ_energy[first_orb][:, None, None] - occ_energy[second_orb][:, None, None])
        amplitude = (live_mask[:, None, None] * intersection / denominator).astype(jnp.bfloat16).astype(jnp.float32)
        contribution = jnp.einsum("pab,xpb->xpa", amplitude, second_fit)
        onehot = (first_slot[:, None] == jnp.arange(owned_count, dtype=jnp.int32)[None, :]).astype(jnp.float32)
        gamma_local = jnp.einsum("xpa,pd->xda", contribution, onehot, precision=lax.Precision.HIGHEST)
        return gamma_local.astype(jnp.bfloat16)

    per_device = lax.map(device_gamma, jnp.arange(N_CLU * N_ORB, dtype=jnp.int32))
    per_device = per_device.reshape(N_CLU, N_ORB, X, owned_count, V)
    cluster_gammas = []
    for cluster in range(N_CLU):
        ordered = jnp.transpose(per_device[cluster], (1, 0, 2, 3)).reshape(X, OCC, V)
        inverse = jnp.argsort(orbital_order[cluster]).astype(jnp.int32)
        cluster_gammas.append(jnp.take(ordered, inverse, axis=1))
    return jnp.concatenate(cluster_gammas, axis=1)
```

```python
import functools

import jax
import jax.numpy as jnp
from jax import lax
from jax.experimental import pallas as pl
from jax.experimental.pallas import tpu as pltpu
from jax.sharding import PartitionSpec as P

MESH = pl.DeviceIdType.MESH
F32 = jnp.float32
BF16 = jnp.bfloat16


def enter(orb, clu):
    barrier = pltpu.get_barrier_semaphore()
    d, c = lax.axis_index("orb"), lax.axis_index("clu")
    me = d * clu + c

    def greet(k, carry):
        to = lax.rem(me + k, orb * clu)
        pl.semaphore_signal(barrier, inc=1, device_id=(to // clu, lax.rem(to, clu)), device_id_type=MESH)
        return carry

    lax.fori_loop(1, orb * clu, greet, 0)
    pl.semaphore_wait(barrier, orb * clu - 1)


def pick_kernel(rows, block, pick_ref, x_ref, out_ref, wide):
    virt = x_ref.shape[2]
    for p in range(block):
        got = jnp.dot(pick_ref[...], x_ref[p], preferred_element_type=F32)
        for lane in range(0, virt, 128):
            wide[lane // 128, pl.ds(p, rows, stride=block), :] = got[:, lane : lane + 128]
    for lane in range(0, virt, 128):
        out_ref[:, :, lane : lane + 128] = wide[lane // 128].reshape(rows, block, 128).astype(BF16)


def place_kernel(rows, block, place_ref, back_ref, out_ref, wide):
    virt = out_ref.shape[2]
    for lane in range(0, virt, 128):
        wide[lane // 128] = back_ref[:, :, lane : lane + 128].astype(F32).reshape(rows * block, 128)
    for q in range(block):
        row = jnp.concatenate(
            [wide[lane // 128, pl.ds(q, rows, stride=block), :] for lane in range(0, virt, 128)], axis=1).astype(BF16)
        out_ref[q] = jnp.dot(place_ref[...], row, preferred_element_type=F32).astype(BF16)


def exchange_kernel(orb, clu, per, xs, table, ve_row, ve_col, picked_ref, mt_ref, back_ref,
                    rows_i, rows_j, mt, fit_i, fit_j, amp, contrib, out,
                    recv_i, recv_j, send_i, send_j, send_j0, recv_back, send_back, m1_send, m1_recv, m2_send, m2_recv):
    d, c = lax.axis_index("orb"), lax.axis_index("clu")
    aux, virt = rows_i.shape[1:]
    slots = clu * per
    width = aux // clu
    chunk = min(256, aux)
    half = min(256, virt)
    mine = pl.ds(pl.multiple_of(d * xs, xs), xs)

    def columns(cluster):
        return pl.ds(pl.multiple_of(cluster * width, width), width)

    def slot_of(t):
        return lax.rem(c + t // per, clu) * per + lax.rem(t, per)

    def second_row(to, cluster, t):
        return picked_ref.at[orb * slots + (to * clu + cluster) * per + lax.rem(t, per)]

    def wait_bytes(ref, sem):
        pltpu.make_async_copy(ref, ref, sem).wait()

    def start_step(t):
        k = t // per
        slot = slot_of(t)
        other = lax.rem(c - k + clu, clu)
        pltpu.make_async_copy(picked_ref.at[d * slots + slot], rows_i.at[t, mine], recv_i.at[t]).start()

        def second(to, sem):
            return pltpu.make_async_remote_copy(
                second_row(to, other, t), rows_j.at[t, mine], sem, recv_j.at[t],
                device_id=(to, other), device_id_type=MESH)

        @pl.when(k == 0)
        def _():
            pltpu.make_async_copy(
                second_row(d, c, t), rows_j.at[t, mine], recv_j.at[t]).start()

        def send(i, carry):
            to = lax.rem(d + i, orb)
            pltpu.make_async_remote_copy(
                picked_ref.at[to * slots + slot], rows_i.at[t, mine], send_i.at[t], recv_i.at[t],
                device_id=(to, c), device_id_type=MESH).start()
            second(to, send_j.at[t]).start()
            return carry

        lax.fori_loop(1, orb, send, 0)

        @pl.when(k != 0)
        def _():
            second(d, send_j0.at[t]).start()

    enter(orb, clu)

    pltpu.make_async_copy(mt_ref.at[:, columns(c)], mt.at[mine, columns(c)], m1_recv.at[0]).start()

    def send_metric(i, carry):
        to = lax.rem(d + i, orb)
        pltpu.make_async_remote_copy(
            mt_ref.at[:, columns(c)], mt.at[mine, columns(c)], m1_send.at[0], m1_recv.at[0],
            device_id=(to, c), device_id_type=MESH).start()
        return carry

    lax.fori_loop(1, orb, send_metric, 0)
    start_step(jnp.int32(0))
    if slots > 1:
        start_step(jnp.int32(1))

    wait_bytes(mt.at[:, columns(c)], m1_recv.at[0])

    def share(cluster, sem):
        return pltpu.make_async_remote_copy(
            mt.at[:, columns(c)], mt.at[:, columns(c)], m2_send.at[cluster], m2_recv.at[sem],
            device_id=(d, cluster), device_id_type=MESH)

    for i in range(1, clu):
        share(lax.rem(c + i, clu), c).start()
    for i in range(1, clu):
        cluster = lax.rem(c + i, clu)
        wait_bytes(mt.at[:, columns(cluster)], m2_recv.at[cluster])

    def step(t, carry):
        slot = slot_of(t)
        wait_bytes(rows_i.at[t], recv_i.at[t])
        wait_bytes(rows_j.at[t], recv_j.at[t])

        @pl.when(t + 2 < slots)
        def _():
            start_step(t + 2)

        def fit(i, carry):
            at = pl.ds(pl.multiple_of(i * chunk, chunk), chunk)
            left = mt[at, :]
            fit_i[at, :] = jnp.dot(left, rows_i[t], preferred_element_type=F32).astype(BF16)
            fit_j[at, :] = jnp.dot(left, rows_j[t], preferred_element_type=F32).astype(BF16)
            return carry

        lax.fori_loop(0, aux // chunk, fit, 0)

        live, occ_i, occ_j = table[slot, 0], table[slot, 1], table[slot, 2]
        for a in range(0, virt, half):
            cross = lax.dot_general(
                fit_i[:, a : a + half], fit_j[...], (((0,), (0,)), ((), ())), preferred_element_type=F32)
            gap = ve_col[a : a + half, :] + ve_row[...] - occ_i - occ_j
            amp[a : a + half, :] = (live * cross / gap).astype(BF16)

        def gamma(i, carry):
            at = pl.ds(pl.multiple_of(i * chunk, chunk), chunk)
            own = lax.dot_general(
                fit_j[at, :], amp[...], (((1,), (1,)), ((), ())), preferred_element_type=F32)
            contrib[t, at, :] = own

            def add(u, total):
                return total + table[slot, 3 + slot_of(u)] * contrib[u, at, :]

            out[t, at, :] = lax.fori_loop(0, t, add, own).astype(BF16)
            return carry

        lax.fori_loop(0, aux // chunk, gamma, 0)

        pltpu.make_async_copy(out.at[t, mine], back_ref.at[d, slot], recv_back.at[t]).start()

        def send_back_to(i, carry):
            to = lax.rem(d + i, orb)
            pltpu.make_async_remote_copy(
                out.at[t, pl.ds(pl.multiple_of(to * xs, xs), xs)], back_ref.at[d, slot],
                send_back.at[t], recv_back.at[t], device_id=(to, c), device_id_type=MESH).start()
            return carry

        lax.fori_loop(1, orb, send_back_to, 0)
        return carry

    lax.fori_loop(0, slots, step, 0)

    others = pl.ds(0, (orb - 1) * xs)
    wait_bytes(mt.at[pl.ds(0, (orb - 1) * xs), columns(c)], m1_send.at[0])
    for i in range(1, clu):
        wait_bytes(mt.at[:, columns(c)], m2_send.at[lax.rem(c + i, clu)])

    def finish(t, carry):
        wait_bytes(rows_i.at[t, others], send_i.at[t])
        wait_bytes(rows_j.at[t, others], send_j.at[t])

        @pl.when(t // per != 0)
        def _():
            wait_bytes(rows_j.at[t, mine], send_j0.at[t])

        wait_bytes(out.at[t, others], send_back.at[t])
        wait_bytes(out.at[t], recv_back.at[t])
        return carry

    lax.fori_loop(0, slots, finish, 0)


def on_device(
    integrals, metric, occ_energy, virt_energy, orbital_order, pair_first, pair_second, pair_live
):
    orb, clu = lax.axis_size("orb"), lax.axis_size("clu")
    d, c = lax.axis_index("orb"), lax.axis_index("clu")
    xs, occ, virt = integrals.shape
    aux = metric.shape[0]
    owned = occ // orb
    slots = pair_second.shape[2]
    per = slots // clu
    any_space = pl.BlockSpec(memory_space=pl.ANY)
    vmem = pl.BlockSpec(memory_space=pltpu.VMEM)
    dma = pltpu.SemaphoreType.DMA

    own_order = lax.dynamic_index_in_dim(orbital_order, c, 0, keepdims=False)
    first_slot = pair_first[0, 0]
    all_first = lax.all_gather(first_slot, "orb", axis=0, tiled=False)
    first_in = jnp.take_along_axis(own_order.reshape(orb, owned), all_first, axis=1)
    wanted = lax.dynamic_slice_in_dim(pair_second, c * per, per, 2).transpose(1, 0, 2)
    index = jnp.concatenate([first_in.reshape(-1), wanted.reshape(-1)])
    numbers = jnp.arange(occ, dtype=jnp.int32)
    pick = (index[:, None] == numbers[None, :]).astype(BF16)
    count = index.shape[0]
    block = min(16, xs)
    picked = pl.pallas_call(
        functools.partial(pick_kernel, count, block),
        grid=(xs // block,),
        out_shape=jax.ShapeDtypeStruct((count, xs, virt), BF16),
        in_specs=[
            pl.BlockSpec((count, occ), lambda i: (0, 0)),
            pl.BlockSpec((block, occ, virt), lambda i: (i, 0, 0)),
        ],
        out_specs=pl.BlockSpec((count, block, virt), lambda i: (0, i, 0)),
        scratch_shapes=[pltpu.VMEM((virt // 128, count * block, 128), F32)],
    )(pick, integrals)

    live = pair_live[0, 0].astype(F32)
    first_orb = lax.dynamic_index_in_dim(first_in, d, 0, keepdims=False) + c * occ
    own_second = lax.dynamic_index_in_dim(
        lax.dynamic_index_in_dim(pair_second, c, 0, keepdims=False), d, 0, keepdims=False)
    second_orb = own_second + jnp.arange(slots, dtype=jnp.int32) // per * occ
    same = (first_slot[:, None] == first_slot[None, :]).astype(F32)
    table = jnp.concatenate(
        [jnp.stack([live, occ_energy[first_orb], occ_energy[second_orb]], axis=1), same], axis=1)

    back = pl.pallas_call(
        functools.partial(exchange_kernel, orb, clu, per, xs),
        out_shape=jax.ShapeDtypeStruct((orb, slots, xs, virt), BF16),
        in_specs=[pl.BlockSpec(memory_space=pltpu.SMEM), vmem, vmem, any_space, any_space],
        out_specs=any_space,
        scratch_shapes=[
            pltpu.VMEM((slots, aux, virt), BF16),
            pltpu.VMEM((slots, aux, virt), BF16),
            pltpu.VMEM((aux, aux), BF16),
            pltpu.VMEM((aux, virt), BF16),
            pltpu.VMEM((aux, virt), BF16),
            pltpu.VMEM((virt, virt), BF16),
            pltpu.VMEM((slots, aux, virt), F32),
            pltpu.VMEM((slots, aux, virt), BF16),
        ] + [dma((slots,))] * 7 + [dma((1,)), dma((1,)), dma((clu,)), dma((clu,))],
        compiler_params=pltpu.CompilerParams(collective_id=0, has_side_effects=True),
    )(table, virt_energy[None, :], virt_energy[:, None], picked, metric.T)

    order = lax.rem(jnp.arange(slots, dtype=jnp.int32) // per - c + clu, clu) * per + jnp.arange(slots) % per
    later = (all_first[:, :, None] == all_first[:, None, :]) & (order[None, None, :] > order[None, :, None])
    speaks = ~jnp.any(later, axis=2)
    place = ((numbers[:, None] == first_in.reshape(-1)[None, :]) & speaks.reshape(-1)[None, :]).astype(BF16)
    count = orb * slots
    return pl.pallas_call(
        functools.partial(place_kernel, count, block),
        grid=(xs // block,),
        out_shape=jax.ShapeDtypeStruct((xs, occ, virt), BF16),
        in_specs=[
            pl.BlockSpec((occ, count), lambda i: (0, 0)),
            pl.BlockSpec((count, block, virt), lambda i: (0, i, 0)),
        ],
        out_specs=pl.BlockSpec((block, occ, virt), lambda i: (i, 0, 0)),
        scratch_shapes=[pltpu.VMEM((virt // 128, count * block, 128), F32)],
    )(place, back.reshape(count, xs, virt))


def solution(mesh):
    in_specs = (
        P("orb", "clu", None),
        P(None, "orb"),
        P(),
        P(),
        P(),
        P("clu", "orb", None),
        P(),
        P("clu", "orb", None),
    )
    out_specs = P("orb", "clu", None)
    return jax.shard_map(
        on_device, mesh=mesh, in_specs=in_specs, out_specs=out_specs, check_vma=False
    )
```
